32 devices in a mesh: img: 2 (over x), rows: 16 (over z, y, core).
Axes of the slice: x: 2, y: 2, z: 4, core: 2. Of those that a mesh axis runs over, the one named last changes fastest.
Arguments:
- image: bfloat16 [128, 256, 512], P(('img', 'rows')), parts along dimension 0, may hold values from -32 to 32
- gain_in: float32 [512], replicated, may hold values from 0.1 to 1.9
- shift_in: float32 [512], replicated, may hold values from -3 to 3
- conv_in: bfloat16 [3, 3, 512, 512], replicated, may hold values from -0.09375 to 0.09375
- gain_mid: float32 [512], replicated, may hold values from 0.1 to 1.9
- shift_mid: float32 [512], replicated, may hold values from -3 to 3
- conv_out: bfloat16 [3, 3, 512, 512], replicated, may hold values from -0.09375 to 0.09375
- bias_out: float32 [512], replicated, may hold values from -2 to 2
Outputs:
- result: bfloat16 [128, 256, 512], P(('img', 'rows')), parts along dimension 0
The draws below stay inside these ranges and needn't reach their ends.
There are 2 independent parts, one for each index of `img`. The reference program is written for one: setup_inputs(seed, part) draws one part's arguments, and reference() takes and returns one part's arrays. A program takes and returns all parts, laid end to end along the dimension named above; an argument that names none is the same for every part. Nothing has to cross between parts.
All inputs are finite; a program needn't handle non-finite values.
Results may differ from the reference program's by a relative error of at most 0.0045.
Values may be sent and summed in bfloat16 or wider, within the bound.
A program may use at most 64 MiB of HBM per device.

```python
import math
import jax
import jax.numpy as jnp
from jax import lax

C = 512
GROUPS = 32
COLS = 256
PICTURE_HEIGHT = 64


def draw_image(key, part):
    sampler_seeds = jax.random.split(key, 8)
    row_pos = jnp.arange(PICTURE_HEIGHT, dtype=jnp.float32) / max(PICTURE_HEIGHT - 1, 1)
    flip = jax.random.uniform(sampler_seeds[4], (), jnp.float32)
    toward = jnp.where(flip < 0.5, row_pos, 1.0 - row_pos)
    log_ratio = jax.random.uniform(sampler_seeds[5], (), jnp.float32, math.log(3.0), math.log(9.0))
    smooth_drift_surface = 1.4 * jnp.exp((toward - 1.0) * log_ratio)
    jagged_surface = jnp.exp(jax.random.uniform(sampler_seeds[6], (PICTURE_HEIGHT,), jnp.float32, math.log(0.7), math.log(1.4)))
    sudden_spike_perturbation = jnp.where(jax.random.uniform(sampler_seeds[7], (PICTURE_HEIGHT,), jnp.float32) < 0.0625, 1.6, 1.0)
    vertical_multiplier = smooth_drift_surface * jagged_surface * sudden_spike_perturbation
    col_scale = jnp.exp(jax.random.uniform(sampler_seeds[0], (COLS,), jnp.float32, math.log(0.3), math.log(3.0)))
    channel_scale_factor = jnp.exp(jax.random.uniform(sampler_seeds[1], (C,), jnp.float32, math.log(0.7), math.log(1.4)))
    noise = jnp.clip(jax.random.normal(sampler_seeds[2], (PICTURE_HEIGHT, COLS, C), jnp.float32), -4.0, 4.0)
    offset = 0.3 * jax.random.normal(sampler_seeds[3], (C,), jnp.float32)
    value_entries = offset + vertical_multiplier[:, None, None] * col_scale[None, :, None] * channel_scale_factor * noise
    return jnp.clip(value_entries, -32.0, 32.0).astype(jnp.bfloat16)


def normal_values(key, dims, deviation, reach, held_as=jnp.bfloat16):
    array = deviation * jax.random.normal(key, dims, jnp.float32)
    return jnp.clip(array, min=-reach, max=reach).astype(held_as)


def setup_inputs(seed: int = 0, part: int = 0) -> dict:
    arg_keys = jax.random.split(jax.random.key(seed), 9)
    own_keys = jax.random.split(jax.random.fold_in(arg_keys[8], part), 9)
    return {
        "image": draw_image(jax.random.fold_in(jax.random.fold_in(arg_keys[8], part), 71), part),
        "gain_in": jnp.clip(1.0 + 0.18 * jax.random.normal(arg_keys[1], (C,), jnp.float32), 0.1, 1.9),
        "shift_in": normal_values(arg_keys[2], (C,), 0.5, 3.0, jnp.float32),
        "conv_in": normal_values(arg_keys[3], (3, 3, C, C), (9 * C) ** -0.5, 0.09375),
        "gain_mid": jnp.clip(1.0 + 0.18 * jax.random.normal(arg_keys[4], (C,), jnp.float32), 0.1, 1.9),
        "shift_mid": normal_values(arg_keys[5], (C,), 0.5, 3.0, jnp.float32),
        "conv_out": normal_values(arg_keys[6], (3, 3, C, C), (9 * C) ** -0.5, 0.09375),
        "bias_out": normal_values(arg_keys[7], (C,), 0.3, 2.0, jnp.float32),
    }


def normalize_silu(value_entries, gain, shift):
    height, width, chans = value_entries.shape
    grouped = value_entries.reshape(height, width, GROUPS, chans // GROUPS)
    midpoint_location = lax.optimization_barrier(jnp.mean(grouped, axis=(0, 1, 3), keepdims=True))
    spread = lax.optimization_barrier(jnp.mean((grouped - midpoint_location) ** 2, axis=(0, 1, 3), keepdims=True))
    scaled = ((grouped - midpoint_location) / jnp.sqrt(spread + 1e-06)).reshape(height, width, chans)
    return jax.nn.silu(scaled * gain + shift).astype(jnp.bfloat16)

def convolve(active, kernel):
    output = lax.conv_general_dilated(active[None].astype(jnp.float32), kernel.astype(jnp.float32), (1, 1), 'SAME', dimension_numbers=('NHWC', 'HWIO', 'NHWC'), precision=lax.Precision.HIGHEST)
    return output[0]

def reference(image, gain_in, shift_in, conv_in, gain_mid, shift_mid, conv_out, bias_out):
    first = normalize_silu(image.astype(jnp.float32), gain_in, shift_in)
    middle = convolve(first, conv_in).astype(jnp.bfloat16)
    latter_operand = normalize_silu(middle.astype(jnp.float32), gain_mid, shift_mid)
    total = image.astype(jnp.float32) + convolve(latter_operand, conv_out) + bias_out
    return total.astype(jnp.bfloat16)
```

```python
import functools

import jax
import jax.numpy as jnp
from jax import lax
from jax.experimental import pallas as pl
from jax.experimental.pallas import tpu as pltpu
from jax.sharding import PartitionSpec as P

GROUPS = 32
LANES = 128
CHUNK = 32
TILE = 256
MESH = pl.DeviceIdType.MESH


def packed(sums, squares):
    chans = sums.shape[1]
    pieces = [part[:, k : k + LANES] for part in (sums, squares) for k in range(0, chans, LANES)]
    return jnp.concatenate(pieces, axis=0)


def flat(tile):
    return jnp.concatenate([tile[k : k + 1] for k in range(tile.shape[0])], axis=1)


def group_total(tile, size):
    lane = lax.broadcasted_iota(jnp.int32, tile.shape, 1)
    step = 1
    while step < size:
        up = pltpu.roll(tile, step, 1)
        down = pltpu.roll(tile, LANES - step, 1)
        tile = tile + jnp.where((lane & step) != 0, up, down)
        step *= 2
    return tile


def kernel(n, image, gain_in, shift_in, conv_in, gain_mid, shift_mid, conv_out, bias_out, out,
           img, act, mid, result, w_in, w_out, acc, gath_in, gath_mid,
           local_sem, out_sem, halo_send, halo_recv, stat_send, stat_recv):
    me = lax.axis_index("rows")
    height, width, chans = image.shape
    count = float(height * width * (chans // GROUPS) * n)
    parts = chans // LANES

    load = pltpu.make_async_copy(image, img.at[pl.ds(1, height)], local_sem.at[0])
    load.start()
    load_w_in = pltpu.make_async_copy(conv_in, w_in, local_sem.at[1])
    load_w_in.start()
    load_w_out = pltpu.make_async_copy(conv_out, w_out, local_sem.at[2])
    load_w_out.start()

    barrier = pltpu.get_barrier_semaphore()
    for d in range(1, n):
        pl.semaphore_signal(
            barrier, inc=1, device_id={"rows": lax.rem(me + d, n)}, device_id_type=MESH
        )

    def add_stats(value, lanes):
        rows = value.shape[0]
        folded = value.reshape(rows // 8, 8, value.shape[1])
        acc[0, :, lanes] += jnp.sum(folded, axis=0)
        acc[1, :, lanes] += jnp.sum(folded * folded, axis=0)

    def stat_copy(gath, which, d):
        return pltpu.make_async_remote_copy(
            src_ref=gath.at[0],
            dst_ref=gath.at[d],
            send_sem=stat_send.at[which, d],
            recv_sem=stat_recv.at[which, d],
            device_id={"rows": lax.rem(me + d, n)},
            device_id_type=MESH,
        )

    def send_stats(gath, which):
        sums = jnp.sum(acc[0], axis=0, keepdims=True)
        squares = jnp.sum(acc[1], axis=0, keepdims=True)
        gath[0] = packed(sums, squares)
        for d in range(1, n):
            stat_copy(gath, which, d).start()

    def receive_stats(gath, which, gain):
        for d in range(1, n):
            stat_copy(gath, which, d).wait()
        total = group_total(jnp.sum(gath[...], axis=0), chans // GROUPS) / count
        mean, square = total[:parts], total[parts:]
        variance = jnp.maximum(square - mean * mean, 0.0)
        return flat(mean), flat(lax.rsqrt(variance + 1e-06)) * gain[...]

    def halo_copies(buf, which):
        up = pltpu.make_async_remote_copy(
            src_ref=buf.at[1],
            dst_ref=buf.at[height + 1],
            send_sem=halo_send.at[which, 0],
            recv_sem=halo_recv.at[which, 0],
            device_id={"rows": jnp.maximum(me - 1, 0)},
            device_id_type=MESH,
        )
        down = pltpu.make_async_remote_copy(
            src_ref=buf.at[height],
            dst_ref=buf.at[0],
            send_sem=halo_send.at[which, 1],
            recv_sem=halo_recv.at[which, 1],
            device_id={"rows": jnp.minimum(me + 1, n - 1)},
            device_id_type=MESH,
        )
        return up, down

    def send_halo(buf, which):
        up, down = halo_copies(buf, which)

        @pl.when(me > 0)
        def _():
            up.start()

        @pl.when(me < n - 1)
        def _():
            down.start()

    def activate(buf, row, mean, scale, shift):
        def step(k, _):
            cols = pl.ds(pl.multiple_of(k * CHUNK, CHUNK), CHUNK)
            half = 0.5 * ((buf[row, cols].astype(jnp.float32) - mean) * scale + shift)
            act[row, cols] = (half + half * jnp.tanh(half)).astype(jnp.bfloat16)
            return 0

        lax.fori_loop(0, width // CHUNK, step, 0, unroll=2)

    def activate_halo(buf, which, mean, scale, shift):
        up, down = halo_copies(buf, which)

        @pl.when(me > 0)
        def _():
            up.wait_send()
            down.wait_recv()
            activate(buf, 0, mean, scale, shift)

        @pl.when(me == 0)
        def _():
            act[0] = jnp.zeros((width, chans), jnp.bfloat16)

        @pl.when(me < n - 1)
        def _():
            down.wait_send()
            up.wait_recv()
            activate(buf, height + 1, mean, scale, shift)

        @pl.when(me == n - 1)
        def _():
            act[height + 1] = jnp.zeros((width, chans), jnp.bfloat16)

    def convolve(rows, weights, finish):
        def step(t, _):
            lanes = pl.ds(pl.multiple_of(t * TILE, TILE), TILE)
            left = jnp.concatenate(
                [jnp.concatenate([act[r + i] for i in range(3)], axis=1) for r in rows], axis=0
            )
            size = left.shape[0]
            y = [
                jnp.dot(
                    left,
                    weights[:, j, :, lanes].reshape(3 * chans, TILE),
                    preferred_element_type=jnp.float32,
                )
                for j in range(3)
            ]
            col = lax.rem(lax.broadcasted_iota(jnp.int32, (size, TILE), 0), width)
            total = y[1] + jnp.where(col == 0, 0.0, pltpu.roll(y[0], 1, 0))
            total = total + jnp.where(col == width - 1, 0.0, pltpu.roll(y[2], size - 1, 0))
            finish(total, lanes)
            return 0

        lax.fori_loop(0, chans // TILE, step, 0)

    acc[...] = jnp.zeros_like(acc)
    load.wait()

    def stats_step(k, _):
        cols = pl.ds(pl.multiple_of(k * CHUNK, CHUNK), CHUNK)
        for r in range(height):
            add_stats(img[1 + r, cols].astype(jnp.float32), slice(None))
        return 0

    lax.fori_loop(0, width // CHUNK, stats_step, 0)
    pl.semaphore_wait(barrier, n - 1)
    send_stats(gath_in, 0)
    send_halo(img, 0)
    acc[...] = jnp.zeros_like(acc)

    inner = [(r, r + 1) for r in range(1, height - 1, 2)]
    outer = (0, height - 1)

    mean, scale = receive_stats(gath_in, 0, gain_in)
    shift = shift_in[...]
    for r in range(1, height + 1):
        activate(img, r, mean, scale, shift)
    load_w_in.wait()

    def keep(rows):
        def finish(total, lanes):
            value = total.astype(jnp.bfloat16)
            add_stats(value.astype(jnp.float32), lanes)
            for k, r in enumerate(rows):
                mid[1 + r, :, lanes] = value[k * width : (k + 1) * width]
        return finish

    for rows in inner:
        convolve(rows, w_in, keep(rows))
    activate_halo(img, 0, mean, scale, shift)
    convolve(outer, w_in, keep(outer))

    send_stats(gath_mid, 1)
    send_halo(mid, 1)
    mean, scale = receive_stats(gath_mid, 1, gain_mid)
    shift = shift_mid[...]
    for r in range(1, height + 1):
        activate(mid, r, mean, scale, shift)
    load_w_out.wait()

    def give(rows):
        def finish(total, lanes):
            bias = bias_out[:, lanes]
            for k, r in enumerate(rows):
                piece = total[k * width : (k + 1) * width] + bias
                piece = img[1 + r, :, lanes].astype(jnp.float32) + piece
                result[r, :, lanes] = piece.astype(jnp.bfloat16)
        return finish

    def store(r):
        return pltpu.make_async_copy(result.at[r], out.at[r], out_sem.at[r])

    for rows in inner:
        convolve(rows, w_out, give(rows))
        for r in rows:
            store(r).start()
    activate_halo(mid, 1, mean, scale, shift)
    convolve(outer, w_out, give(outer))
    for r in outer:
        store(r).start()
    for r in range(height):
        store(r).wait()


def local(n, image, gain_in, shift_in, conv_in, gain_mid, shift_mid, conv_out, bias_out):
    height, width, chans = image.shape
    whole = pl.BlockSpec(memory_space=pl.ANY)
    vector = pl.BlockSpec(memory_space=pltpu.VMEM)
    bf16, f32 = jnp.bfloat16, jnp.float32
    rows = 2 * chans // LANES
    return pl.pallas_call(
        functools.partial(kernel, n),
        out_shape=jax.ShapeDtypeStruct(image.shape, image.dtype),
        in_specs=[whole, vector, vector, whole, vector, vector, whole, vector],
        out_specs=whole,
        scratch_shapes=[
            pltpu.VMEM((height + 2, width, chans), bf16),
            pltpu.VMEM((height + 2, width, chans), bf16),
            pltpu.VMEM((height + 2, width, chans), bf16),
            pltpu.VMEM((height, width, chans), bf16),
            pltpu.VMEM(conv_in.shape, bf16),
            pltpu.VMEM(conv_out.shape, bf16),
            pltpu.VMEM((2, 8, chans), f32),
            pltpu.VMEM((n, rows, LANES), f32),
            pltpu.VMEM((n, rows, LANES), f32),
            pltpu.SemaphoreType.DMA((3,)),
            pltpu.SemaphoreType.DMA((height,)),
            pltpu.SemaphoreType.DMA((2, 2)),
            pltpu.SemaphoreType.DMA((2, 2)),
            pltpu.SemaphoreType.DMA((2, n)),
            pltpu.SemaphoreType.DMA((2, n)),
        ],
        compiler_params=pltpu.CompilerParams(
            collective_id=0, has_side_effects=True, vmem_limit_bytes=60 * 1024 * 1024
        ),
    )(image, gain_in[None], shift_in[None], conv_in, gain_mid[None], shift_mid[None], conv_out,
      bias_out[None])


def solution(mesh):
    n = mesh.shape["rows"]
    in_specs = (P(("img", "rows"), None, None), P(), P(), P(), P(), P(), P(), P())
    out_specs = P(("img", "rows"), None, None)
    return jax.shard_map(
        functools.partial(local, n), mesh=mesh, in_specs=in_specs, out_specs=out_specs,
        check_vma=False,
    )
```

```python
import functools

import jax
import jax.numpy as jnp
from jax import lax
from jax.experimental import pallas as pl
from jax.experimental.pallas import tpu as pltpu
from jax.sharding import PartitionSpec as P

GROUPS = 32
LANES = 128
CHUNK = 32
TILE = 256
MESH = pl.DeviceIdType.MESH


def packed(sums, squares):
    chans = sums.shape[1]
    pieces = [part[:, k : k + LANES] for part in (sums, squares) for k in range(0, chans, LANES)]
    return jnp.concatenate(pieces, axis=0)


def flat(tile):
    return jnp.concatenate([tile[k : k + 1] for k in range(tile.shape[0])], axis=1)


def group_total(tile, size):
    lane = lax.broadcasted_iota(jnp.int32, tile.shape, 1)
    step = 1
    while step < size:
        up = pltpu.roll(tile, step, 1)
        down = pltpu.roll(tile, LANES - step, 1)
        tile = tile + jnp.where((lane & step) != 0, up, down)
        step *= 2
    return tile


def kernel(n, image, gain_in, shift_in, conv_in, gain_mid, shift_mid, conv_out, bias_out, out,
           img, act, mid, result, w_in, w_out, w_mix, v_mix, acc, gath_in, gath_mid,
           local_sem, out_sem, halo_send, halo_recv, stat_send, stat_recv):
    me = lax.axis_index("rows")
    height, width, chans = image.shape
    count = float(height * width * (chans // GROUPS) * n)
    parts = chans // LANES

    load = pltpu.make_async_copy(image, img.at[pl.ds(1, height)], local_sem.at[0])
    load.start()
    load_w_in = pltpu.make_async_copy(conv_in, w_in, local_sem.at[1])
    load_w_in.start()
    load_w_out = pltpu.make_async_copy(conv_out, w_out, local_sem.at[2])
    load_w_out.start()

    barrier = pltpu.get_barrier_semaphore()
    for d in range(1, n):
        pl.semaphore_signal(
            barrier, inc=1, device_id={"rows": lax.rem(me + d, n)}, device_id_type=MESH
        )

    def add_stats(value, lanes):
        rows = value.shape[0]
        folded = value.reshape(rows // 8, 8, value.shape[1])
        acc[0, :, lanes] += jnp.sum(folded, axis=0)
        acc[1, :, lanes] += jnp.sum(folded * folded, axis=0)

    def stat_copy(gath, which, d):
        return pltpu.make_async_remote_copy(
            src_ref=gath.at[0],
            dst_ref=gath.at[d],
            send_sem=stat_send.at[which, d],
            recv_sem=stat_recv.at[which, d],
            device_id={"rows": lax.rem(me + d, n)},
            device_id_type=MESH,
        )

    def send_stats(gath, which):
        sums = jnp.sum(acc[0], axis=0, keepdims=True)
        squares = jnp.sum(acc[1], axis=0, keepdims=True)
        gath[0] = packed(sums, squares)
        for d in range(1, n):
            stat_copy(gath, which, d).start()

    def receive_stats(gath, which, gain):
        for d in range(1, n):
            stat_copy(gath, which, d).wait()
        total = group_total(jnp.sum(gath[...], axis=0), chans // GROUPS) / count
        mean, square = total[:parts], total[parts:]
        variance = jnp.maximum(square - mean * mean, 0.0)
        return flat(mean), flat(lax.rsqrt(variance + 1e-06)) * (0.5 * gain[...])

    def halo_copies(buf, which):
        up = pltpu.make_async_remote_copy(
            src_ref=buf.at[1],
            dst_ref=buf.at[height + 1],
            send_sem=halo_send.at[which, 0],
            recv_sem=halo_recv.at[which, 0],
            device_id={"rows": jnp.maximum(me - 1, 0)},
            device_id_type=MESH,
        )
        down = pltpu.make_async_remote_copy(
            src_ref=buf.at[height],
            dst_ref=buf.at[0],
            send_sem=halo_send.at[which, 1],
            recv_sem=halo_recv.at[which, 1],
            device_id={"rows": jnp.minimum(me + 1, n - 1)},
            device_id_type=MESH,
        )
        return up, down

    def send_halo(buf, which):
        up, down = halo_copies(buf, which)

        @pl.when(me > 0)
        def _():
            up.start()

        @pl.when(me < n - 1)
        def _():
            down.start()

    def activate(buf, row, mean, scale, shift):
        def step(k, _):
            cols = pl.ds(pl.multiple_of(k * CHUNK, CHUNK), CHUNK)
            half = (buf[row, cols].astype(jnp.float32) - mean) * scale + shift
            act[row, cols] = (half + half * jnp.tanh(half)).astype(jnp.bfloat16)
            return 0

        lax.fori_loop(0, width // CHUNK, step, 0, unroll=2)

    def activate_halo(buf, which, mean, scale, shift):
        up, down = halo_copies(buf, which)

        @pl.when(me > 0)
        def _():
            up.wait_send()
            down.wait_recv()
            activate(buf, 0, mean, scale, shift)

        @pl.when(me == 0)
        def _():
            act[0] = jnp.zeros((width, chans), jnp.bfloat16)

        @pl.when(me < n - 1)
        def _():
            down.wait_send()
            up.wait_recv()
            activate(buf, height + 1, mean, scale, shift)

        @pl.when(me == n - 1)
        def _():
            act[height + 1] = jnp.zeros((width, chans), jnp.bfloat16)

    def combine(y):
        size = y[0].shape[0]
        col = lax.rem(lax.broadcasted_iota(jnp.int32, y[0].shape, 0), width)
        total = y[1] + jnp.where(col == 0, 0.0, pltpu.roll(y[0], 1, 0))
        return total + jnp.where(col == width - 1, 0.0, pltpu.roll(y[2], size - 1, 0))

    def mix_weights():
        def step(k, _):
            taps = pl.ds(pl.multiple_of(k * CHUNK, CHUNK), CHUNK)
            for j in range(3):
                ends = 0.5 * (
                    w_out[0, j, taps].astype(jnp.float32) + w_out[2, j, taps].astype(jnp.float32)
                )
                centre = 0.5 * w_out[1, j, taps].astype(jnp.float32)
                w_mix[0, j, taps] = (ends + centre).astype(jnp.bfloat16)
                w_mix[1, j, taps] = (ends - centre).astype(jnp.bfloat16)
            return 0

        lax.fori_loop(0, chans // CHUNK, step, 0)

    def convolve_pair(row, finish):
        def mix(k, _):
            cols = pl.ds(pl.multiple_of(k * CHUNK, CHUNK), CHUNK)
            d = [act[row + i, cols].astype(jnp.float32) for i in range(4)]
            for i, value in enumerate((d[0] - d[2], d[1] + d[2], d[2] - d[1], d[1] - d[3])):
                v_mix[i, cols] = value.astype(jnp.bfloat16)
            return 0

        lax.fori_loop(0, width // CHUNK, mix, 0, unroll=2)

        def step(t, _):
            lanes = pl.ds(pl.multiple_of(t * TILE, TILE), TILE)
            taps = (w_out.at[0], w_mix.at[0], w_mix.at[1], w_out.at[2])
            y = [
                [
                    jnp.dot(v_mix[i], taps[i][j, :, lanes], preferred_element_type=jnp.float32)
                    for j in range(3)
                ]
                for i in range(4)
            ]
            part = [combine(products) for products in y]
            first = part[0] + (part[1] + part[2])
            second = (part[1] - part[2]) - part[3]
            finish(jnp.concatenate([first, second], axis=0), lanes)
            return 0

        lax.fori_loop(0, chans // TILE, step, 0)

    def convolve(rows, weights, finish):
        def step(t, _):
            lanes = pl.ds(pl.multiple_of(t * TILE, TILE), TILE)
            left = jnp.concatenate(
                [jnp.concatenate([act[r + i] for i in range(3)], axis=1) for r in rows], axis=0
            )
            y = [
                jnp.dot(
                    left,
                    weights[:, j, :, lanes].reshape(3 * chans, TILE),
                    preferred_element_type=jnp.float32,
                )
                for j in range(3)
            ]
            total = combine(y)
            finish(total, lanes)
            return 0

        lax.fori_loop(0, chans // TILE, step, 0)

    acc[...] = jnp.zeros_like(acc)
    load.wait()

    def stats_step(k, _):
        cols = pl.ds(pl.multiple_of(k * CHUNK, CHUNK), CHUNK)
        for r in range(height):
            add_stats(img[1 + r, cols].astype(jnp.float32), slice(None))
        return 0

    lax.fori_loop(0, width // CHUNK, stats_step, 0)
    pl.semaphore_wait(barrier, n - 1)
    send_stats(gath_in, 0)
    send_halo(img, 0)
    acc[...] = jnp.zeros_like(acc)

    inner = [(r, r + 1) for r in range(1, height - 1, 2)]
    outer = (0, height - 1)

    load_w_out.wait()
    mix_weights()
    mean, scale = receive_stats(gath_in, 0, gain_in)
    shift = 0.5 * shift_in[...]
    for r in range(1, height + 1):
        activate(img, r, mean, scale, shift)
    load_w_in.wait()

    def keep(rows):
        def finish(total, lanes):
            value = total.astype(jnp.bfloat16)
            add_stats(value.astype(jnp.float32), lanes)
            for k, r in enumerate(rows):
                mid[1 + r, :, lanes] = value[k * width : (k + 1) * width]
        return finish

    for rows in inner:
        convolve(rows, w_in, keep(rows))
    activate_halo(img, 0, mean, scale, shift)
    convolve(outer, w_in, keep(outer))

    send_stats(gath_mid, 1)
    send_halo(mid, 1)
    mean, scale = receive_stats(gath_mid, 1, gain_mid)
    shift = 0.5 * shift_mid[...]
    for r in range(1, height + 1):
        activate(mid, r, mean, scale, shift)

    def give(rows):
        def finish(total, lanes):
            bias = bias_out[:, lanes]
            for k, r in enumerate(rows):
                piece = total[k * width : (k + 1) * width] + bias
                piece = img[1 + r, :, lanes].astype(jnp.float32) + piece
                result[r, :, lanes] = piece.astype(jnp.bfloat16)
        return finish

    def store(r):
        return pltpu.make_async_copy(result.at[r], out.at[r], out_sem.at[r])

    for rows in inner:
        convolve_pair(rows[0], give(rows))
        for r in rows:
            store(r).start()
    activate_halo(mid, 1, mean, scale, shift)
    convolve(outer, w_out, give(outer))
    for r in outer:
        store(r).start()
    for r in range(height):
        store(r).wait()


def local(n, image, gain_in, shift_in, conv_in, gain_mid, shift_mid, conv_out, bias_out):
    height, width, chans = image.shape
    whole = pl.BlockSpec(memory_space=pl.ANY)
    vector = pl.BlockSpec(memory_space=pltpu.VMEM)
    bf16, f32 = jnp.bfloat16, jnp.float32
    rows = 2 * chans // LANES
    return pl.pallas_call(
        functools.partial(kernel, n),
        out_shape=jax.ShapeDtypeStruct(image.shape, image.dtype),
        in_specs=[whole, vector, vector, whole, vector, vector, whole, vector],
        out_specs=whole,
        scratch_shapes=[
            pltpu.VMEM((height + 2, width, chans), bf16),
            pltpu.VMEM((height + 2, width, chans), bf16),
            pltpu.VMEM((height + 2, width, chans), bf16),
            pltpu.VMEM((height, width, chans), bf16),
            pltpu.VMEM(conv_in.shape, bf16),
            pltpu.VMEM(conv_out.shape, bf16),
            pltpu.VMEM((2,) + conv_out.shape[1:], bf16),
            pltpu.VMEM((4, width, chans), bf16),
            pltpu.VMEM((2, 8, chans), f32),
            pltpu.VMEM((n, rows, LANES), f32),
            pltpu.VMEM((n, rows, LANES), f32),
            pltpu.SemaphoreType.DMA((3,)),
            pltpu.SemaphoreType.DMA((height,)),
            pltpu.SemaphoreType.DMA((2, 2)),
            pltpu.SemaphoreType.DMA((2, 2)),
            pltpu.SemaphoreType.DMA((2, n)),
            pltpu.SemaphoreType.DMA((2, n)),
        ],
        compiler_params=pltpu.CompilerParams(
            collective_id=0, has_side_effects=True, vmem_limit_bytes=60 * 1024 * 1024
        ),
    )(image, gain_in[None], shift_in[None], conv_in, gain_mid[None], shift_mid[None], conv_out,
      bias_out[None])


def solution(mesh):
    n = mesh.shape["rows"]
    in_specs = (P(("img", "rows"), None, None), P(), P(), P(), P(), P(), P(), P())
    out_specs = P(("img", "rows"), None, None)
    return jax.shard_map(
        functools.partial(local, n), mesh=mesh, in_specs=in_specs, out_specs=out_specs,
        check_vma=False,
    )
```
